32 devices in a mesh: wide: 4 (over x, core), narrow: 8 (over z, y).
Axes of the slice: x: 2, y: 2, z: 4, core: 2. Of those that a mesh axis runs over, the one named last changes fastest.
Arguments:
- resid_in: bfloat16 [4096, 4096], P('wide', 'narrow'), may hold values from -6 to 6
- low_feat: bfloat16 [4096, 4096], P('wide', 'narrow'), may hold values from -6 to 6
- mid_feat: bfloat16 [4096, 4096], P('wide', 'narrow'), may hold values from -6 to 6
- segment: int32 [4096], P('wide'), may hold values from 0 to 31, never falling along the last dimension, each value on 1 to 256 neighbouring positions
- assign: int32 [4, 4], replicated, may hold values from 0 to 3, each once within a row
- attn_gain: float32 [4096], replicated, may hold values from 0.25 to 1.75
- qk_gain: float32 [2, 128], replicated, may hold values from 0.5 to 9
- query_weight: bfloat16 [4096, 4096], P(None, 'narrow'), may hold values from -0.09375 to 0.09375
- kv_weight: bfloat16 [4096, 512], P(None, 'narrow'), may hold values from -0.09375 to 0.09375
- out_weight: bfloat16 [4096, 4096], P('narrow'), may hold values from -0.09375 to 0.09375
- joining_weight: float32 [12288, 4096], P('wide', 'narrow'), may hold values from -0.0546875 to 0.0546875
- momentum: float32 [12288, 4096], P('wide', 'narrow'), may hold values from -0.06 to 0.06
Outputs:
- draft_error: float32 [4096, 4096], P('wide', 'narrow')
- new_joining: float32 [12288, 4096], P('wide', 'narrow')
- new_momentum: float32 [12288, 4096], P('wide', 'narrow')
The draws below stay inside these ranges and needn't reach their ends.
Inputs may be any that keep to these rules, and one draw needn't show every extreme that they name: Each row of assign names every draft group exactly once. `segment`: ids never fall along the tokens.
All inputs are finite; a program needn't handle non-finite values.
Results may differ from the reference program's by a relative error of at most 0.004.
The reference program's roundings to bfloat16 on the way count: a program that leaves them out, or rounds other values in their place, can miss the bound.
Values may be sent and summed in bfloat16 or wider, within the bound.
No kernel may reach another device: no remote copies, remote signals or barrier semaphores. Data moves between devices by JAX's collectives and lax.ppermute only.
A program may use at most 192 MiB of HBM per device.

```python
import math
import jax
import jax.numpy as jnp
import numpy as np
from jax import lax

D = 4096
HEADS = 32
KVH = 2
HD = 128
TOK_GRP = 1024
TOKENS = 4096
N_WIDE = 4


def draw_qk_gain(key, part):
    uniform_draw = jax.random.uniform(key, (2, HD), jnp.float32)
    lower_end = jnp.log(0.5)
    upper_end = jnp.log(2.0)
    return jnp.exp(lower_end + uniform_draw * (upper_end - lower_end))


def block_scale(stream_key, extent, pieces, low, high):
    factor_of = 1.0
    for axis_at, shards_of in pieces:
        draws = jax.random.uniform(jax.random.fold_in(jax.random.fold_in(stream_key, 6), axis_at), (shards_of,), jnp.float32, low / len(pieces), high / len(pieces))
        factor_of = factor_of * jnp.repeat(jnp.exp(draws), extent[axis_at] // shards_of).reshape((-1,) + (1,) * (len(extent) - 1 - axis_at))
    return factor_of


def length_profile(number_of, total, most, slope):
    portions = [(1 << 20) // math.isqrt(rank ** slope) + 1 for rank in range(2, number_of + 1)]
    spare, counts = total - most - (number_of - 1), [1] * (number_of - 1)
    while spare > 0:
        free = [i for i in range(number_of - 1) if counts[i] < most]
        pool, budget = sum([portions[i] for i in free]), spare
        for i in free:
            addition = min(most - counts[i], max(1, budget * portions[i] // pool), spare)
            counts[i] = counts[i] + addition
            spare = spare - addition
    return np.array([most] + counts)


def ragged(stream_key, number_of, total, most, slope):
    if number_of == 2:
        one = jax.random.randint(stream_key, (), max(1, total - most), min(most, total - 1) + 1)
        return jnp.stack([one, total - one])
    tallies = jnp.asarray(length_profile(number_of, total, most, slope), jnp.int32)
    couples = (number_of - 1) // 2
    donor, sink = tallies[1:1 + 2 * couples:2], tallies[2:2 + 2 * couples:2]
    room = jnp.minimum(donor - 1, most - sink)
    moved = jax.random.randint(jax.random.fold_in(stream_key, 1), (couples,), 0, 1 << 20) % (room + 1)
    tallies = tallies.at[1:1 + 2 * couples:2].set(donor - moved).at[2:2 + 2 * couples:2].set(sink + moved)
    return tallies[jax.random.permutation(jax.random.fold_in(stream_key, 2), number_of)]


def centred(own_key, shape, scale, limit, shards=(), held_as=jnp.bfloat16):
    level = block_scale(own_key, shape, shards, -0.22, 0.18) if shards else 1.0
    drawn = jax.random.normal(own_key, shape, jnp.float32) * scale * level
    return jnp.minimum(jnp.maximum(drawn, -limit), limit).astype(held_as)


def setup_inputs(seed: int = 0) -> dict:
    arg_keys = jax.random.split(jax.random.key(seed), 13)
    return {
        "resid_in": centred(arg_keys[0], (TOKENS, D), 1.0, 6.0, ((0, 4), (1, 8))),
        "low_feat": centred(arg_keys[1], (TOKENS, D), 1.0, 6.0, ((0, 4), (1, 8))),
        "mid_feat": centred(arg_keys[2], (TOKENS, D), 1.0, 6.0, ((0, 4), (1, 8))),
        "segment": jnp.searchsorted(jnp.cumsum(ragged(arg_keys[3], max(TOKENS // 128, 8), TOKENS, min(256, TOK_GRP), 1)), jnp.arange(TOKENS), side="right").astype(jnp.int32),
        "assign": jax.vmap(lambda own: jax.random.permutation(own, N_WIDE))(jax.random.split(arg_keys[4], N_WIDE)).reshape((N_WIDE, N_WIDE)).astype(jnp.int32),
        "attn_gain": jnp.clip(1.0 + 0.15 * jax.random.normal(arg_keys[5], (D,), jnp.float32), 0.25, 1.75),
        "qk_gain": draw_qk_gain(jax.random.fold_in(arg_keys[12], 71), 0),
        "query_weight": centred(arg_keys[7], (D, HEADS * HD), D ** -0.5, 0.09375, ((1, 8),)),
        "kv_weight": centred(arg_keys[8], (D, 2 * KVH * HD), D ** -0.5, 0.09375, ((1, 8),)),
        "out_weight": centred(arg_keys[9], (HEADS * HD, D), (HEADS * HD) ** -0.5, 0.09375, ((0, 8),)),
        "joining_weight": centred(arg_keys[10], (3 * D, D), (3 * D) ** -0.5, 0.0546875, ((0, 4), (1, 8)), jnp.float32),
        "momentum": centred(arg_keys[11], (3 * D, D), 0.01, 0.06, ((0, 4), (1, 8)), jnp.float32),
    }


mom_decay = 0.9
step_size = 0.5

def rms_scale(values, gain):
    return values * lax.rsqrt(lax.optimization_barrier(jnp.mean(values * values, axis=-1, keepdims=True)) + 1e-06) * gain

def reference(resid_in, low_feat, mid_feat, segment, assign, attn_gain, qk_gain, query_weight, kv_weight, out_weight, joining_weight, momentum):
    per_head = HEADS // KVH
    width_kv = KVH * HD
    block = TOK_GRP // N_WIDE
    features = []
    targets = []
    masks = []
    for group in range(N_WIDE):
        lower = group * TOK_GRP
        hidden = resid_in[lower:lower + TOK_GRP].astype(jnp.float32)
        normed = rms_scale(hidden, attn_gain).astype(jnp.bfloat16)
        queries = jnp.dot(normed, query_weight, preferred_element_type=jnp.float32).reshape(TOK_GRP, HEADS, HD)
        queries = rms_scale(queries, qk_gain[0]).astype(jnp.bfloat16)
        keyvals = jnp.dot(normed, kv_weight, preferred_element_type=jnp.float32).astype(jnp.bfloat16)
        keyvals = lax.optimization_barrier(keyvals).astype(jnp.float32)
        keys = rms_scale(keyvals[:, :width_kv].reshape(TOK_GRP, KVH, HD), qk_gain[1]).astype(jnp.bfloat16)
        value_heads = keyvals[:, width_kv:].reshape(TOK_GRP, KVH, HD)
        keys_all = jnp.repeat(keys, per_head, axis=1).astype(jnp.float32)
        values_all = jnp.repeat(value_heads, per_head, axis=1)
        scores = jnp.einsum('qhd,khd->hqk', queries.astype(jnp.float32), keys_all) * HD ** (-0.5)
        seg_group = segment[lower:lower + TOK_GRP]
        positions = jnp.arange(TOK_GRP)
        allowed = (positions[:, None] >= positions[None, :]) & (seg_group[:, None] == seg_group[None, :])
        scores = jnp.where(allowed[None], scores, jnp.float32(-1e+30))
        highest = lax.optimization_barrier(jnp.max(scores, axis=-1, keepdims=True))
        expd = jnp.exp(scores - highest)
        probs = (expd / lax.optimization_barrier(jnp.sum(expd, axis=-1, keepdims=True))).astype(jnp.bfloat16)
        context = jnp.einsum('hqk,khd->qhd', probs.astype(jnp.float32), values_all)
        context = context.astype(jnp.bfloat16).reshape(TOK_GRP, HEADS * HD)
        high = hidden + jnp.dot(context, out_weight, preferred_element_type=jnp.float32)
        valid = jnp.concatenate([(seg_group[1:] == seg_group[:-1]).astype(jnp.float32), jnp.zeros((1,), jnp.float32)])
        shifted = jnp.concatenate([high[1:], jnp.zeros((1, D), jnp.float32)], axis=0) * valid[:, None]
        targets.append(shifted.astype(jnp.bfloat16))
        masks.append(valid.astype(jnp.bfloat16))
        features.append(jnp.concatenate([low_feat[lower:lower + TOK_GRP], mid_feat[lower:lower + TOK_GRP], high.astype(jnp.bfloat16)], axis=1))
    slots = jnp.arange(N_WIDE, dtype=jnp.int32)
    inverse = lax.optimization_barrier(jnp.sum(jnp.where(assign[:, None, :] == slots[None, :, None], slots[None, None, :], 0), axis=2)).astype(jnp.int32)
    joined_bf = joining_weight.astype(jnp.bfloat16)
    grads = jnp.zeros((3 * D, D), jnp.float32)
    errors = []
    for draft in range(N_WIDE):
        input_parts = []
        target_parts = []
        mask_parts = []
        for group in range(N_WIDE):
            start = (inverse[group, draft] * block).astype(jnp.int32)
            input_parts.append(lax.dynamic_slice_in_dim(features[group], start, block, 0))
            target_parts.append(lax.dynamic_slice_in_dim(targets[group], start, block, 0))
            mask_parts.append(lax.dynamic_slice_in_dim(masks[group], start, block, 0))
        inputs = jnp.concatenate(input_parts, axis=0)
        target = jnp.concatenate(target_parts, axis=0).astype(jnp.float32)
        valid = jnp.concatenate(mask_parts, axis=0).astype(jnp.float32)
        pred = jnp.dot(inputs, joined_bf, preferred_element_type=jnp.float32)
        error = (pred - target) * valid[:, None]
        errors.append(error)
        grads = grads + lax.dot_general(inputs, error.astype(jnp.bfloat16), (((0,), (0,)), ((), ())), preferred_element_type=jnp.float32)
    grads = grads / TOKENS
    new_momentum = mom_decay * momentum + grads
    new_joining = joining_weight - step_size * new_momentum
    return (jnp.concatenate(errors, axis=0), new_joining, new_momentum)
```

```python
import math

import jax
import jax.numpy as jnp
from jax import lax
from jax.experimental import pallas as pl
from jax.experimental.pallas import tpu as pltpu
from jax.sharding import PartitionSpec as P


KVH = 2
HD = 128
LONGEST = 256


mom_decay = 0.9
step_size = 0.5


def rms_scale(values, gain):
    return values * lax.rsqrt(jnp.mean(values * values, axis=-1, keepdims=True) + 1e-06) * gain


def ring_order(count):
    return list(range(0, count, 2)) + list(range(count - 1 - count % 2, 0, -2))


def ring_gather(shard, axis, base, extra, beside):
    count = lax.axis_size(axis)
    order = ring_order(count)
    place = [0] * count
    for at, member in enumerate(order):
        place[member] = at
    ahead = [(order[i], order[(i + 1) % count]) for i in range(count)]
    back = [(b, a) for a, b in ahead]
    own = lax.axis_index(axis)
    here = jnp.asarray(place, jnp.int32)[own]
    ring = jnp.asarray(order, jnp.int32)
    rows, width = shard.shape
    half = rows // 2
    parts = [shard[:half], shard[half:]]
    full = lax.dynamic_update_slice(base, shard, (0, own * width))
    moving = {(way, part): parts[part] for way in (0, 1) for part in (0, 1)}
    there = ring[(here + jnp.arange(count)) % count]
    for step in range(1, count // 2 + 1):
        last = count // 2 - step
        fresh = []
        for part in (0, 1):
            for way in (0, 1):
                if step == count // 2 and way != part:
                    continue
                got = lax.ppermute(moving[way, part], axis, back if way else ahead)
                source = ring[(here + step if way else here - step) % count]
                fresh.append((way, part, got, source))
        if last in beside:
            extra = beside[last](extra, full, there)
            extra, *held = lax.optimization_barrier((extra, *[item[2] for item in fresh]))
            fresh = [(way, part, got, source) for (way, part, _, source), got in zip(fresh, held)]
        for way, part, got, source in fresh:
            moving[way, part] = got
            full = lax.dynamic_update_slice(full, got, (part * half, source * width))
    return full, extra, there


def listed_gather(shard, axis):
    order = ring_order(lax.axis_size(axis))
    return lax.all_gather(shard, axis, axis=1, tiled=True, axis_index_groups=[order])


def wide_pieces(shard, axis):
    count = lax.axis_size(axis)
    pieces = [shard]
    for k in range(1, count):
        bit = k & -k
        pieces.append(lax.ppermute(pieces[k & (k - 1)], axis, [(i, i ^ bit) for i in range(count)]))
    return pieces


def head_pieces(part, axis):
    count = lax.axis_size(axis)
    share = count // KVH
    split = share // 2
    own = lax.axis_index(axis)

    def source(head, q):
        return head * split + q if q < split else KVH * split + head * split + q - split

    got = []
    for turn in range(share):
        perm = [
            (source(head, (j + turn) % share), head * share + j)
            for head in range(KVH)
            for j in range(share)
        ]
        got.append(lax.ppermute(part, axis, perm))
    stacked = jnp.stack(got + got)
    ordered = lax.dynamic_slice_in_dim(stacked, (share - own % share) % share, share, 0)
    rows = part.shape[0]
    key = jnp.swapaxes(ordered[:split], 0, 1).reshape(rows, HD)
    value = jnp.swapaxes(ordered[split:], 0, 1).reshape(rows, HD)
    return key, value


def project(hidden, order, gain, query_weight, kv_weight, head_gains):
    tokens, features = hidden.shape
    cols = query_weight.shape[1]
    width = features // len(order)
    rows = math.gcd(tokens, 256)

    def body(hidden_ref, gain_ref, query_ref, kv_ref, head_ref, q_ref, k_ref, v_ref):
        total = jnp.zeros((rows, 1), jnp.float32)
        for at in range(len(order)):
            values = hidden_ref[:, at * width : (at + 1) * width].astype(jnp.float32)
            total = total + jnp.sum(values * values, axis=-1, keepdims=True)
        scale = lax.rsqrt(total / features + 1e-06)
        product = jnp.zeros((rows, cols), jnp.float32)
        keyval = jnp.zeros((rows, 2 * HD), jnp.float32)
        for at, member in enumerate(order):
            values = hidden_ref[:, at * width : (at + 1) * width].astype(jnp.float32)
            picked = slice(member * width, (member + 1) * width)
            normed = (values * scale * gain_ref[:, picked]).astype(jnp.bfloat16)
            product = product + jnp.dot(
                normed, query_ref[picked, :], preferred_element_type=jnp.float32
            )
            keyval = keyval + jnp.dot(
                normed, kv_ref[picked, :], preferred_element_type=jnp.float32
            )
        for head in range(cols // HD):
            lanes = slice(head * HD, (head + 1) * HD)
            q_ref[:, lanes] = rms_scale(product[:, lanes], head_ref[0:1, :]).astype(jnp.bfloat16)
        keyval = keyval.astype(jnp.bfloat16)
        v_ref[...] = keyval[:, HD:]
        key = keyval[:, :HD].astype(jnp.float32)
        k_ref[...] = rms_scale(key, head_ref[1:2, :]).astype(jnp.bfloat16)

    whole = lambda i: (0, 0)
    row = lambda i: (i, 0)
    return pl.pallas_call(
        body,
        grid=(tokens // rows,),
        in_specs=[
            pl.BlockSpec((rows, features), row),
            pl.BlockSpec((1, features), whole),
            pl.BlockSpec((features, cols), whole),
            pl.BlockSpec((features, 2 * HD), whole),
            pl.BlockSpec((2, HD), whole),
        ],
        out_specs=[
            pl.BlockSpec((rows, cols), row),
            pl.BlockSpec((rows, HD), row),
            pl.BlockSpec((rows, HD), row),
        ],
        out_shape=[
            jax.ShapeDtypeStruct((tokens, cols), jnp.bfloat16),
            jax.ShapeDtypeStruct((tokens, HD), jnp.bfloat16),
            jax.ShapeDtypeStruct((tokens, HD), jnp.bfloat16),
        ],
        cost_estimate=pl.CostEstimate(
            flops=2 * tokens * features * (cols + 2 * HD),
            transcendentals=0,
            bytes_accessed=2 * tokens * features,
        ),
        name="project",
    )(hidden, gain.reshape(1, features), query_weight, kv_weight, head_gains)


def attend(queries, key, value, segment):
    tokens, cols = queries.shape
    rows = math.gcd(tokens, LONGEST) if tokens % LONGEST else LONGEST
    assert rows == LONGEST

    def body(q_ref, k0_ref, k1_ref, v0_ref, v1_ref, col_ref, row0_ref, row1_ref, out_ref):
        at = pl.program_id(0)
        kept = []
        for back, (k_ref, row_ref) in ((1, (k0_ref, row0_ref)), (0, (k1_ref, row1_ref))):
            keys = k_ref[...]
            ours = lax.broadcasted_iota(jnp.int32, (rows, rows), 0)
            theirs = lax.broadcasted_iota(jnp.int32, (rows, rows), 1) - back * rows
            allowed = (ours >= theirs) & (theirs + at * rows >= 0) & (col_ref[...] == row_ref[...])
            kept.append((keys, allowed))
        for head in range(cols // HD):
            lanes = slice(head * HD, (head + 1) * HD)
            query = q_ref[:, lanes]
            scores = []
            for keys, allowed in kept:
                score = lax.dot_general(
                    query, keys, (((1,), (1,)), ((), ())), preferred_element_type=jnp.float32
                )
                scores.append(jnp.where(allowed, score * HD ** (-0.5), jnp.float32(-1e30)))
            highest = jnp.maximum(
                jnp.max(scores[0], axis=-1, keepdims=True),
                jnp.max(scores[1], axis=-1, keepdims=True),
            )
            expd = [jnp.exp(score - highest) for score in scores]
            norm = jnp.sum(expd[0], axis=-1, keepdims=True) + jnp.sum(
                expd[1], axis=-1, keepdims=True
            )
            probs = [(e / norm).astype(jnp.bfloat16) for e in expd]
            context = jnp.dot(
                probs[0], v0_ref[...], preferred_element_type=jnp.float32
            ) + jnp.dot(probs[1], v1_ref[...], preferred_element_type=jnp.float32)
            out_ref[:, lanes] = context.astype(jnp.bfloat16)

    before = lambda i: (jnp.maximum(i - 1, 0), 0)
    current = lambda i: (i, 0)
    before_row = lambda i: (0, jnp.maximum(i - 1, 0))
    current_row = lambda i: (0, i)
    return pl.pallas_call(
        body,
        grid=(tokens // rows,),
        in_specs=[
            pl.BlockSpec((rows, cols), current),
            pl.BlockSpec((rows, HD), before),
            pl.BlockSpec((rows, HD), current),
            pl.BlockSpec((rows, HD), before),
            pl.BlockSpec((rows, HD), current),
            pl.BlockSpec((rows, 1), current),
            pl.BlockSpec((1, rows), before_row),
            pl.BlockSpec((1, rows), current_row),
        ],
        out_specs=pl.BlockSpec((rows, cols), current),
        out_shape=jax.ShapeDtypeStruct((tokens, cols), jnp.bfloat16),
        cost_estimate=pl.CostEstimate(
            flops=32 * tokens * rows * cols, transcendentals=0, bytes_accessed=4 * tokens * cols
        ),
        name="attend",
    )(
        queries,
        key,
        key,
        value,
        value,
        segment.reshape(tokens, 1),
        segment.reshape(1, tokens),
        segment.reshape(1, tokens),
    )


def predict(feat, places, table, joined, first, base, target=None, valid=None):
    tokens = feat.shape[0]
    steps = table.shape[0]
    inner = feat.shape[1] // lax.axis_size("narrow")
    cols = joined.shape[1]
    ends = target is not None

    def body(places_ref, table_ref, *refs):
        at = pl.program_id(0)
        feat_ref, joined_ref = refs[:2]
        out_ref = refs[-2] if ends else refs[-1]
        product = jnp.dot(feat_ref[...], joined_ref[...], preferred_element_type=jnp.float32)

        @pl.when(at == 0)
        def _():
            out_ref[...] = product if base is None else refs[2][...] + product

        @pl.when(at > 0)
        def _():
            out_ref[...] += product

        if ends:

            @pl.when(at == steps - 1)
            def _():
                error = (out_ref[...] - refs[3][...].astype(jnp.float32)) * refs[4][...]
                out_ref[...] = error
                refs[-1][...] = error.astype(jnp.bfloat16)

    whole = lambda i, places_ref, table_ref: (0, 0)
    in_specs = [
        pl.BlockSpec((tokens, inner), lambda i, places_ref, table_ref: (0, places_ref[i])),
        pl.BlockSpec(
            (inner, cols), lambda i, places_ref, table_ref: (first // inner + table_ref[i], 0)
        ),
    ]
    operands = [feat, joined]
    if base is not None:
        in_specs.append(pl.BlockSpec((tokens, cols), whole))
        operands.append(base)
    out_specs = pl.BlockSpec((tokens, cols), whole)
    out_shape = jax.ShapeDtypeStruct((tokens, cols), jnp.float32)
    if ends:
        in_specs += [pl.BlockSpec((tokens, cols), whole), pl.BlockSpec((tokens, 1), whole)]
        operands += [target, valid.reshape(tokens, 1)]
        out_specs = [out_specs, pl.BlockSpec((tokens, cols), whole)]
        out_shape = [out_shape, jax.ShapeDtypeStruct((tokens, cols), jnp.bfloat16)]
    return pl.pallas_call(
        body,
        grid_spec=pltpu.PrefetchScalarGridSpec(
            num_scalar_prefetch=2, grid=(steps,), in_specs=in_specs, out_specs=out_specs
        ),
        out_shape=out_shape,
        cost_estimate=pl.CostEstimate(
            flops=2 * tokens * steps * inner * cols,
            transcendentals=0,
            bytes_accessed=2 * tokens * steps * inner,
        ),
        name="predict",
    )(places, table, *operands)


def grad_rows(first, pieces, width, tables, feats, errors, out_dtype):
    per = tables[0].shape[0]
    kinds = len(tables)
    tokens, cols = errors[0].shape

    def body(first_ref, table_ref, *refs):
        out_ref = refs[-1]
        error_refs = refs[-1 - len(errors) : -1]
        piece = first_ref[0] + pl.program_id(0)
        for at in range(kinds):

            @pl.when(piece // per == at)
            def _(at=at):
                total = None
                for group, error_ref in enumerate(error_refs):
                    term = lax.dot_general(
                        refs[group * kinds + at][...],
                        error_ref[...],
                        (((0,), (0,)), ((), ())),
                        preferred_element_type=jnp.float32,
                    )
                    total = term if total is None else total + term
                out_ref[...] = total.astype(out_dtype)

    def feat_map(at):
        def of(i, first_ref, table_ref):
            piece = jnp.clip(first_ref[0] + i - at * per, 0, per - 1)
            return (0, table_ref[at * per + piece])

        return of

    whole = lambda i, first_ref, table_ref: (0, 0)
    in_specs = [
        pl.BlockSpec((tokens, width), feat_map(at)) for _ in errors for at in range(kinds)
    ]
    in_specs += [pl.BlockSpec((tokens, cols), whole) for _ in errors]
    return pl.pallas_call(
        body,
        grid_spec=pltpu.PrefetchScalarGridSpec(
            num_scalar_prefetch=2,
            grid=(pieces,),
            in_specs=in_specs,
            out_specs=pl.BlockSpec((width, cols), lambda i, first_ref, table_ref: (i, 0)),
        ),
        out_shape=jax.ShapeDtypeStruct((pieces * width, cols), out_dtype),
        cost_estimate=pl.CostEstimate(
            flops=4 * tokens * pieces * width * cols,
            transcendentals=0,
            bytes_accessed=4 * tokens * pieces * width,
        ),
        name="grad_rows",
    )(first.reshape(1), jnp.concatenate(tables), *[f for group in feats for f in group], *errors)


def step_on_device(
    resid_in,
    low_feat,
    mid_feat,
    segment,
    assign,
    attn_gain,
    qk_gain,
    query_weight,
    kv_weight,
    out_weight,
    joining_weight,
    momentum,
):
    groups = lax.axis_size("wide")
    narrow = lax.axis_size("narrow")
    mine = lax.axis_index("wide").astype(jnp.int32)
    tokens_local = resid_in.shape[0]
    block = tokens_local // groups
    features = query_weight.shape[0]
    width = features // narrow
    order = ring_order(narrow)
    partner = [(i, i ^ 1) for i in range(groups)]

    hidden_full = listed_gather(resid_in, "narrow")
    low_full = listed_gather(low_feat, "narrow")
    mid_full = listed_gather(mid_feat, "narrow")

    share = out_weight.shape[0] // groups
    rows_mine = lax.dynamic_slice_in_dim(out_weight, mine * share, share, 0)
    got = lax.all_to_all(rows_mine, "narrow", split_axis=1, concat_axis=0, tiled=True)
    out_pieces = wide_pieces(got, "wide")
    rows_here = joining_weight.shape[0]
    joined_pieces = wide_pieces(joining_weight.astype(jnp.bfloat16), "wide")

    kv_share = features // groups
    kv_rows = lax.dynamic_slice_in_dim(kv_weight, mine * kv_share, kv_share, 0)
    kv_rows = jnp.concatenate(head_pieces(kv_rows, "narrow"), axis=1)
    kv_own = jnp.zeros((features, 2 * HD), kv_weight.dtype)
    for k, piece in enumerate(wide_pieces(kv_rows, "wide")):
        kv_own = lax.dynamic_update_slice(kv_own, piece, ((mine ^ k) * kv_share, 0))

    hidden_full, kv_own, joined_pieces, out_pieces = lax.optimization_barrier(
        (hidden_full, kv_own, joined_pieces, out_pieces)
    )
    out_cols = jnp.zeros((narrow, groups, share, width), out_weight.dtype)
    for k, piece in enumerate(out_pieces):
        out_cols = lax.dynamic_update_slice(
            out_cols, piece.reshape(narrow, 1, share, width), (0, mine ^ k, 0, 0)
        )
    out_cols = out_cols.reshape(narrow * groups * share, width)
    joined = jnp.zeros((rows_here * groups, joining_weight.shape[1]), jnp.bfloat16)
    for k, piece in enumerate(joined_pieces):
        joined = lax.dynamic_update_slice(joined, piece, ((mine ^ k) * rows_here, 0))

    queries, key, value = project(
        hidden_full, order, attn_gain, query_weight, kv_own, qk_gain
    )
    context = attend(queries, key, value, segment)

    listed = jnp.asarray(order, jnp.int32)
    natural = jnp.arange(narrow, dtype=jnp.int32)
    low_other = lax.ppermute(low_full, "wide", partner)
    mid_other = lax.ppermute(mid_full, "wide", partner)

    def of_low(pred, full, there):
        return predict(low_full, natural, listed, joined, 0, None)

    def of_mid(pred, full, there):
        return predict(mid_full, natural, listed, joined, features, pred)

    def of_high(pred, full, there):
        near = jnp.concatenate([there[: narrow // 2], there[narrow // 2 + 1 :]])
        return predict(full, near, near, joined, 2 * features, pred)

    context_full, pred, _ = ring_gather(context, "narrow", hidden_full, None, {1: of_low})
    attn_cols = jnp.dot(context_full, out_cols, preferred_element_type=jnp.float32)
    high = resid_in.astype(jnp.float32) + attn_cols
    valid = jnp.concatenate(
        [(segment[1:] == segment[:-1]).astype(jnp.float32), jnp.zeros((1,), jnp.float32)]
    )
    target = (
        jnp.concatenate([high[1:], jnp.zeros((1, high.shape[1]), jnp.float32)], axis=0)
        * valid[:, None]
    ).astype(jnp.bfloat16)
    high_full, pred, there = ring_gather(
        high.astype(jnp.bfloat16), "narrow", context_full, pred, {1: of_mid, 0: of_high}
    )
    last = there[narrow // 2 : narrow // 2 + 1]
    high_other = lax.ppermute(high_full, "wide", partner)

    error, error_bf = predict(
        high_full, last, last, joined, 2 * features, pred, target, valid
    )
    error_other = lax.ppermute(error_bf, "wide", partner)

    own_row = assign[mine]
    slots = jnp.arange(groups, dtype=jnp.int32)
    inverse = jnp.sum(jnp.where(own_row[None, :] == slots[:, None], slots[None, :], 0), axis=1)
    sent = []
    for k in sorted(range(groups), key=lambda k: -k):
        piece = lax.dynamic_slice_in_dim(error, inverse[mine ^ k] * block, block, 0)
        if k:
            piece = lax.ppermute(piece, "wide", [(i, i ^ k) for i in range(groups)])
        sent.append((k, piece))

    place = jnp.asarray([order.index(member) for member in range(narrow)], jnp.int32)
    tables = (place, place, natural)
    feats = ((low_full, mid_full, high_full), (low_other, mid_other, high_other))
    per_chunk = rows_here // width

    def rows_of(member, dtype):
        return grad_rows(
            member * per_chunk, per_chunk, width, tables, feats, (error_bf, error_other), dtype
        )

    far = []
    for bit in range(2, groups, 2):
        away = rows_of(mine ^ bit, jnp.bfloat16)
        far.append(lax.ppermute(away, "wide", [(i, i ^ bit) for i in range(groups)]))
    grads = rows_of(mine, jnp.float32)
    error_out = jnp.zeros_like(error)
    for k, piece in sent:
        error_out = lax.dynamic_update_slice(error_out, piece, ((mine ^ k) * block, 0))
    for piece in far:
        grads = grads + piece.astype(jnp.float32)
    grads = grads / (tokens_local * groups)
    new_momentum = mom_decay * momentum + grads
    new_joining = joining_weight - step_size * new_momentum
    return (error_out, new_joining, new_momentum)


def solution(mesh):
    placed = (
        P("wide", "narrow"),
        P("wide", "narrow"),
        P("wide", "narrow"),
        P("wide"),
        P(),
        P(),
        P(),
        P(None, "narrow"),
        P(None, "narrow"),
        P("narrow", None),
        P("wide", "narrow"),
        P("wide", "narrow"),
    )
    return jax.shard_map(
        step_on_device,
        mesh=mesh,
        in_specs=placed,
        out_specs=(P("wide", "narrow"), P("wide", "narrow"), P("wide", "narrow")),
        check_vma=False,
    )
```

```python
import math

import jax
import jax.numpy as jnp
from jax import lax
from jax.experimental import pallas as pl
from jax.experimental.pallas import tpu as pltpu
from jax.sharding import PartitionSpec as P


KVH = 2
HD = 128
LONGEST = 256


mom_decay = 0.9
step_size = 0.5


def rms_scale(values, gain):
    return values * lax.rsqrt(jnp.mean(values * values, axis=-1, keepdims=True) + 1e-06) * gain


def ring_order(count):
    return list(range(0, count, 2)) + list(range(count - 1 - count % 2, 0, -2))


def ring_gather(shard, axis, base, extra, beside):
    count = lax.axis_size(axis)
    order = ring_order(count)
    place = [0] * count
    for at, member in enumerate(order):
        place[member] = at
    ahead = [(order[i], order[(i + 1) % count]) for i in range(count)]
    back = [(b, a) for a, b in ahead]
    own = lax.axis_index(axis)
    here = jnp.asarray(place, jnp.int32)[own]
    ring = jnp.asarray(order, jnp.int32)
    rows, width = shard.shape
    half = rows // 2
    parts = [shard[:half], shard[half:]]
    full = lax.dynamic_update_slice(base, shard, (0, own * width))
    moving = {(way, part): parts[part] for way in (0, 1) for part in (0, 1)}
    there = ring[(here + jnp.arange(count)) % count]
    for step in range(1, count // 2 + 1):
        last = count // 2 - step
        fresh = []
        for part in (0, 1):
            for way in (0, 1):
                if step == count // 2 and way != part:
                    continue
                got = lax.ppermute(moving[way, part], axis, back if way else ahead)
                source = ring[(here + step if way else here - step) % count]
                fresh.append((way, part, got, source))
        if last in beside:
            extra = beside[last](extra, full, there)
            extra, *held = lax.optimization_barrier((extra, *[item[2] for item in fresh]))
            fresh = [(way, part, got, source) for (way, part, _, source), got in zip(fresh, held)]
        for way, part, got, source in fresh:
            moving[way, part] = got
            full = lax.dynamic_update_slice(full, got, (part * half, source * width))
    return full, extra, there


def listed_gather(shard, axis):
    order = ring_order(lax.axis_size(axis))
    return lax.all_gather(shard, axis, axis=1, tiled=True, axis_index_groups=[order])


def wide_pieces(shard, axis):
    count = lax.axis_size(axis)
    pieces = [shard]
    for k in range(1, count):
        bit = k & -k
        pieces.append(lax.ppermute(pieces[k & (k - 1)], axis, [(i, i ^ bit) for i in range(count)]))
    return pieces


def head_pieces(part, axis):
    count = lax.axis_size(axis)
    share = count // KVH
    split = share // 2
    own = lax.axis_index(axis)

    def source(head, q):
        return head * split + q if q < split else KVH * split + head * split + q - split

    got = []
    for turn in range(share):
        perm = [
            (source(head, (j + turn) % share), head * share + j)
            for head in range(KVH)
            for j in range(share)
        ]
        got.append(lax.ppermute(part, axis, perm))
    stacked = jnp.stack(got + got)
    ordered = lax.dynamic_slice_in_dim(stacked, (share - own % share) % share, share, 0)
    rows = part.shape[0]
    key = jnp.swapaxes(ordered[:split], 0, 1).reshape(rows, HD)
    value = jnp.swapaxes(ordered[split:], 0, 1).reshape(rows, HD)
    return key, value


def project(hidden, order, gain, query_weight, kv_weight, head_gains):
    tokens, features = hidden.shape
    cols = query_weight.shape[1]
    width = features // len(order)
    rows = math.gcd(tokens, 256)

    def body(hidden_ref, gain_ref, query_ref, kv_ref, head_ref, q_ref, k_ref, v_ref):
        total = jnp.zeros((rows, 1), jnp.float32)
        for at in range(len(order)):
            values = hidden_ref[:, at * width : (at + 1) * width].astype(jnp.float32)
            total = total + jnp.sum(values * values, axis=-1, keepdims=True)
        scale = lax.rsqrt(total / features + 1e-06)
        product = jnp.zeros((rows, cols), jnp.float32)
        keyval = jnp.zeros((rows, 2 * HD), jnp.float32)
        for at, member in enumerate(order):
            values = hidden_ref[:, at * width : (at + 1) * width].astype(jnp.float32)
            picked = slice(member * width, (member + 1) * width)
            normed = (values * scale * gain_ref[:, picked]).astype(jnp.bfloat16)
            product = product + jnp.dot(
                normed, query_ref[picked, :], preferred_element_type=jnp.float32
            )
            keyval = keyval + jnp.dot(
                normed, kv_ref[picked, :], preferred_element_type=jnp.float32
            )
        for head in range(cols // HD):
            lanes = slice(head * HD, (head + 1) * HD)
            q_ref[:, lanes] = rms_scale(product[:, lanes], head_ref[0:1, :]).astype(jnp.bfloat16)
        keyval = keyval.astype(jnp.bfloat16)
        v_ref[...] = keyval[:, HD:]
        key = keyval[:, :HD].astype(jnp.float32)
        k_ref[...] = rms_scale(key, head_ref[1:2, :]).astype(jnp.bfloat16)

    whole = lambda i: (0, 0)
    row = lambda i: (i, 0)
    return pl.pallas_call(
        body,
        grid=(tokens // rows,),
        in_specs=[
            pl.BlockSpec((rows, features), row),
            pl.BlockSpec((1, features), whole),
            pl.BlockSpec((features, cols), whole),
            pl.BlockSpec((features, 2 * HD), whole),
            pl.BlockSpec((2, HD), whole),
        ],
        out_specs=[
            pl.BlockSpec((rows, cols), row),
            pl.BlockSpec((rows, HD), row),
            pl.BlockSpec((rows, HD), row),
        ],
        out_shape=[
            jax.ShapeDtypeStruct((tokens, cols), jnp.bfloat16),
            jax.ShapeDtypeStruct((tokens, HD), jnp.bfloat16),
            jax.ShapeDtypeStruct((tokens, HD), jnp.bfloat16),
        ],
        cost_estimate=pl.CostEstimate(
            flops=2 * tokens * features * (cols + 2 * HD),
            transcendentals=0,
            bytes_accessed=2 * tokens * features,
        ),
        name="project",
    )(hidden, gain.reshape(1, features), query_weight, kv_weight, head_gains)


def attend(queries, key, value, segment):
    tokens, cols = queries.shape
    rows = math.gcd(tokens, LONGEST) if tokens % LONGEST else LONGEST
    assert rows == LONGEST

    def body(q_ref, k0_ref, k1_ref, v0_ref, v1_ref, col_ref, row0_ref, row1_ref, out_ref):
        at = pl.program_id(0)
        kept = []
        for back, (k_ref, row_ref) in ((1, (k0_ref, row0_ref)), (0, (k1_ref, row1_ref))):
            keys = k_ref[...]
            ours = lax.broadcasted_iota(jnp.int32, (rows, rows), 0)
            theirs = lax.broadcasted_iota(jnp.int32, (rows, rows), 1) - back * rows
            allowed = (ours >= theirs) & (theirs + at * rows >= 0) & (col_ref[...] == row_ref[...])
            kept.append((keys, allowed))
        for head in range(cols // HD):
            lanes = slice(head * HD, (head + 1) * HD)
            query = q_ref[:, lanes]
            scores = []
            for keys, allowed in kept:
                score = lax.dot_general(
                    query, keys, (((1,), (1,)), ((), ())), preferred_element_type=jnp.float32
                )
                scores.append(jnp.where(allowed, score * HD ** (-0.5), jnp.float32(-1e30)))
            highest = jnp.maximum(
                jnp.max(scores[0], axis=-1, keepdims=True),
                jnp.max(scores[1], axis=-1, keepdims=True),
            )
            expd = [jnp.exp(score - highest) for score in scores]
            norm = jnp.sum(expd[0], axis=-1, keepdims=True) + jnp.sum(
                expd[1], axis=-1, keepdims=True
            )
            probs = [(e / norm).astype(jnp.bfloat16) for e in expd]
            context = jnp.dot(
                probs[0], v0_ref[...], preferred_element_type=jnp.float32
            ) + jnp.dot(probs[1], v1_ref[...], preferred_element_type=jnp.float32)
            out_ref[:, lanes] = context.astype(jnp.bfloat16)

    before = lambda i: (jnp.maximum(i - 1, 0), 0)
    current = lambda i: (i, 0)
    before_row = lambda i: (0, jnp.maximum(i - 1, 0))
    current_row = lambda i: (0, i)
    return pl.pallas_call(
        body,
        grid=(tokens // rows,),
        in_specs=[
            pl.BlockSpec((rows, cols), current),
            pl.BlockSpec((rows, HD), before),
            pl.BlockSpec((rows, HD), current),
            pl.BlockSpec((rows, HD), before),
            pl.BlockSpec((rows, HD), current),
            pl.BlockSpec((rows, 1), current),
            pl.BlockSpec((1, rows), before_row),
            pl.BlockSpec((1, rows), current_row),
        ],
        out_specs=pl.BlockSpec((rows, cols), current),
        out_shape=jax.ShapeDtypeStruct((tokens, cols), jnp.bfloat16),
        cost_estimate=pl.CostEstimate(
            flops=32 * tokens * rows * cols, transcendentals=0, bytes_accessed=4 * tokens * cols
        ),
        name="attend",
    )(
        queries,
        key,
        key,
        value,
        value,
        segment.reshape(tokens, 1),
        segment.reshape(1, tokens),
        segment.reshape(1, tokens),
    )


def predict(feat, places, table, joined, first, base, target=None, valid=None):
    tokens = feat.shape[0]
    steps = table.shape[0]
    inner = feat.shape[1] // lax.axis_size("narrow")
    cols = joined.shape[1]
    ends = target is not None

    def body(places_ref, table_ref, *refs):
        at = pl.program_id(0)
        feat_ref, joined_ref = refs[:2]
        out_ref = refs[-2] if ends else refs[-1]
        product = jnp.dot(feat_ref[...], joined_ref[...], preferred_element_type=jnp.float32)

        @pl.when(at == 0)
        def _():
            out_ref[...] = product if base is None else refs[2][...] + product

        @pl.when(at > 0)
        def _():
            out_ref[...] += product

        if ends:

            @pl.when(at == steps - 1)
            def _():
                error = (out_ref[...] - refs[3][...].astype(jnp.float32)) * refs[4][...]
                out_ref[...] = error
                refs[-1][...] = error.astype(jnp.bfloat16)

    whole = lambda i, places_ref, table_ref: (0, 0)
    in_specs = [
        pl.BlockSpec((tokens, inner), lambda i, places_ref, table_ref: (0, places_ref[i])),
        pl.BlockSpec(
            (inner, cols), lambda i, places_ref, table_ref: (first // inner + table_ref[i], 0)
        ),
    ]
    operands = [feat, joined]
    if base is not None:
        in_specs.append(pl.BlockSpec((tokens, cols), whole))
        operands.append(base)
    out_specs = pl.BlockSpec((tokens, cols), whole)
    out_shape = jax.ShapeDtypeStruct((tokens, cols), jnp.float32)
    if ends:
        in_specs += [pl.BlockSpec((tokens, cols), whole), pl.BlockSpec((tokens, 1), whole)]
        operands += [target, valid.reshape(tokens, 1)]
        out_specs = [out_specs, pl.BlockSpec((tokens, cols), whole)]
        out_shape = [out_shape, jax.ShapeDtypeStruct((tokens, cols), jnp.bfloat16)]
    return pl.pallas_call(
        body,
        grid_spec=pltpu.PrefetchScalarGridSpec(
            num_scalar_prefetch=2, grid=(steps,), in_specs=in_specs, out_specs=out_specs
        ),
        out_shape=out_shape,
        cost_estimate=pl.CostEstimate(
            flops=2 * tokens * steps * inner * cols,
            transcendentals=0,
            bytes_accessed=2 * tokens * steps * inner,
        ),
        name="predict",
    )(places, table, *operands)


def grad_rows(first, pieces, parts, width, tables, feats, errors, out_dtype):
    per = tables[0].shape[0]
    kinds = len(tables)
    tokens, cols = errors[0].shape
    each = pieces // parts

    def body(first_ref, table_ref, *refs):
        out_refs = refs[-parts:]
        error_refs = refs[-parts - len(errors) : -parts]
        piece = first_ref[0] + pl.program_id(0)
        for at in range(kinds):

            @pl.when(piece // per == at)
            def _(at=at):
                total = None
                for group, error_ref in enumerate(error_refs):
                    term = lax.dot_general(
                        refs[group * kinds + at][...],
                        error_ref[...],
                        (((0,), (0,)), ((), ())),
                        preferred_element_type=jnp.float32,
                    )
                    total = term if total is None else total + term
                for part, out_ref in enumerate(out_refs):

                    @pl.when(pl.program_id(0) // each == part)
                    def _(out_ref=out_ref):
                        out_ref[...] = total.astype(out_dtype)

    def out_map(part):
        return lambda i, first_ref, table_ref: (jnp.clip(i - part * each, 0, each - 1), 0)

    def feat_map(at):
        def of(i, first_ref, table_ref):
            piece = jnp.clip(first_ref[0] + i - at * per, 0, per - 1)
            return (0, table_ref[at * per + piece])

        return of

    whole = lambda i, first_ref, table_ref: (0, 0)
    in_specs = [
        pl.BlockSpec((tokens, width), feat_map(at)) for _ in errors for at in range(kinds)
    ]
    in_specs += [pl.BlockSpec((tokens, cols), whole) for _ in errors]
    return pl.pallas_call(
        body,
        grid_spec=pltpu.PrefetchScalarGridSpec(
            num_scalar_prefetch=2,
            grid=(pieces,),
            in_specs=in_specs,
            out_specs=[pl.BlockSpec((width, cols), out_map(part)) for part in range(parts)],
        ),
        out_shape=[jax.ShapeDtypeStruct((each * width, cols), out_dtype)] * parts,
        cost_estimate=pl.CostEstimate(
            flops=4 * tokens * pieces * width * cols,
            transcendentals=0,
            bytes_accessed=4 * tokens * pieces * width,
        ),
        name="grad_rows",
    )(first.reshape(1), jnp.concatenate(tables), *[f for group in feats for f in group], *errors)


def update(grads, far, joining, momentum, part, outs, tokens):
    rows, cols = far[0].shape
    step = math.gcd(rows, 256)
    skip = part * (rows // step)

    def body(grads_ref, joining_ref, momentum_ref, *refs):
        total = grads_ref[...]
        for far_ref in refs[: len(far)]:
            total = total + far_ref[...].astype(jnp.float32)
        fresh = mom_decay * momentum_ref[...] + total / tokens
        refs[-2][...] = joining_ref[...] - step_size * fresh
        refs[-1][...] = fresh

    here = pl.BlockSpec((step, cols), lambda i: (skip + i, 0))
    own = pl.BlockSpec((step, cols), lambda i: (i, 0))
    shape = jax.ShapeDtypeStruct(joining.shape, jnp.float32)
    return pl.pallas_call(
        body,
        grid=(rows // step,),
        in_specs=[here] * 3
        + [own] * len(far)
        + [pl.BlockSpec(memory_space=pl.ANY)] * len(outs),
        out_specs=[here, here],
        out_shape=[shape, shape],
        input_output_aliases={3 + len(far) + at: at for at in range(len(outs))},
        cost_estimate=pl.CostEstimate(
            flops=6 * rows * cols, transcendentals=0, bytes_accessed=22 * rows * cols
        ),
        name="update",
    )(grads, joining, momentum, *far, *outs)


def step_on_device(
    resid_in,
    low_feat,
    mid_feat,
    segment,
    assign,
    attn_gain,
    qk_gain,
    query_weight,
    kv_weight,
    out_weight,
    joining_weight,
    momentum,
):
    groups = lax.axis_size("wide")
    narrow = lax.axis_size("narrow")
    mine = lax.axis_index("wide").astype(jnp.int32)
    tokens_local = resid_in.shape[0]
    block = tokens_local // groups
    features = query_weight.shape[0]
    width = features // narrow
    order = ring_order(narrow)
    partner = [(i, i ^ 1) for i in range(groups)]

    hidden_full = listed_gather(resid_in, "narrow")
    low_full = listed_gather(low_feat, "narrow")
    mid_full = listed_gather(mid_feat, "narrow")

    share = out_weight.shape[0] // groups
    rows_mine = lax.dynamic_slice_in_dim(out_weight, mine * share, share, 0)
    got = lax.all_to_all(rows_mine, "narrow", split_axis=1, concat_axis=0, tiled=True)
    out_pieces = wide_pieces(got, "wide")
    rows_here = joining_weight.shape[0]
    joined_pieces = wide_pieces(joining_weight.astype(jnp.bfloat16), "wide")

    kv_share = features // groups
    kv_rows = lax.dynamic_slice_in_dim(kv_weight, mine * kv_share, kv_share, 0)
    kv_rows = jnp.concatenate(head_pieces(kv_rows, "narrow"), axis=1)
    kv_own = jnp.zeros((features, 2 * HD), kv_weight.dtype)
    for k, piece in enumerate(wide_pieces(kv_rows, "wide")):
        kv_own = lax.dynamic_update_slice(kv_own, piece, ((mine ^ k) * kv_share, 0))

    hidden_full, kv_own, joined_pieces, out_pieces = lax.optimization_barrier(
        (hidden_full, kv_own, joined_pieces, out_pieces)
    )
    out_cols = jnp.zeros((narrow, groups, share, width), out_weight.dtype)
    for k, piece in enumerate(out_pieces):
        out_cols = lax.dynamic_update_slice(
            out_cols, piece.reshape(narrow, 1, share, width), (0, mine ^ k, 0, 0)
        )
    out_cols = out_cols.reshape(narrow * groups * share, width)
    joined = jnp.zeros((rows_here * groups, joining_weight.shape[1]), jnp.bfloat16)
    for k, piece in enumerate(joined_pieces):
        joined = lax.dynamic_update_slice(joined, piece, ((mine ^ k) * rows_here, 0))

    queries, key, value = project(
        hidden_full, order, attn_gain, query_weight, kv_own, qk_gain
    )
    context = attend(queries, key, value, segment)

    listed = jnp.asarray(order, jnp.int32)
    natural = jnp.arange(narrow, dtype=jnp.int32)
    low_other = lax.ppermute(low_full, "wide", partner)
    mid_other = lax.ppermute(mid_full, "wide", partner)

    def of_low(pred, full, there):
        return predict(low_full, natural, listed, joined, 0, None)

    def of_mid(pred, full, there):
        return predict(mid_full, natural, listed, joined, features, pred)

    def of_high(pred, full, there):
        near = jnp.concatenate([there[: narrow // 2], there[narrow // 2 + 1 :]])
        return predict(full, near, near, joined, 2 * features, pred)

    context_full, pred, _ = ring_gather(context, "narrow", hidden_full, None, {1: of_low})
    attn_cols = jnp.dot(context_full, out_cols, preferred_element_type=jnp.float32)
    high = resid_in.astype(jnp.float32) + attn_cols
    valid = jnp.concatenate(
        [(segment[1:] == segment[:-1]).astype(jnp.float32), jnp.zeros((1,), jnp.float32)]
    )
    target = (
        jnp.concatenate([high[1:], jnp.zeros((1, high.shape[1]), jnp.float32)], axis=0)
        * valid[:, None]
    ).astype(jnp.bfloat16)
    high_full, pred, there = ring_gather(
        high.astype(jnp.bfloat16), "narrow", context_full, pred, {1: of_mid, 0: of_high}
    )
    last = there[narrow // 2 : narrow // 2 + 1]
    high_other = lax.ppermute(high_full, "wide", partner)

    error, error_bf = predict(
        high_full, last, last, joined, 2 * features, pred, target, valid
    )
    error_other = lax.ppermute(error_bf, "wide", partner)

    own_row = assign[mine]
    slots = jnp.arange(groups, dtype=jnp.int32)
    inverse = jnp.sum(jnp.where(own_row[None, :] == slots[:, None], slots[None, :], 0), axis=1)
    sent = []
    for k in sorted(range(groups), key=lambda k: -k):
        piece = lax.dynamic_slice_in_dim(error, inverse[mine ^ k] * block, block, 0)
        if k > 1:
            piece = piece.astype(jnp.bfloat16)
        if k:
            piece = lax.ppermute(piece, "wide", [(i, i ^ k) for i in range(groups)])
        sent.append((k, piece))

    place = jnp.asarray([order.index(member) for member in range(narrow)], jnp.int32)
    tables = (place, place, natural)
    feats = ((low_full, mid_full, high_full), (low_other, mid_other, high_other))
    per_chunk = rows_here // width

    def rows_of(member, parts, dtype):
        return grad_rows(
            member * per_chunk,
            per_chunk,
            parts,
            width,
            tables,
            feats,
            (error_bf, error_other),
            dtype,
        )

    parts = 2
    far = []
    for bit in range(2, groups, 2):
        away = rows_of(mine ^ bit, parts, jnp.bfloat16)
        moved = []
        for piece in away:
            moved.append(lax.ppermute(piece, "wide", [(i, i ^ bit) for i in range(groups)]))
        far.append(moved)
    (grads,) = rows_of(mine, 1, jnp.float32)
    error_out = jnp.zeros_like(error)
    for k, piece in sent:
        error_out = lax.dynamic_update_slice(
            error_out, piece.astype(jnp.float32), ((mine ^ k) * block, 0)
        )
    outs = ()
    for part in range(parts):
        pieces = [moved[part] for moved in far]
        outs = update(
            grads, pieces, joining_weight, momentum, part, outs, tokens_local * groups
        )
    new_joining, new_momentum = outs
    return (error_out, new_joining, new_momentum)


def solution(mesh):
    placed = (
        P("wide", "narrow"),
        P("wide", "narrow"),
        P("wide", "narrow"),
        P("wide"),
        P(),
        P(),
        P(),
        P(None, "narrow"),
        P(None, "narrow"),
        P("narrow", None),
        P("wide", "narrow"),
        P("wide", "narrow"),
    )
    return jax.shard_map(
        step_on_device,
        mesh=mesh,
        in_specs=placed,
        out_specs=(P("wide", "narrow"), P("wide", "narrow"), P("wide", "narrow")),
        check_vma=False,
    )
```

```python
import math

import jax
import jax.numpy as jnp
from jax import lax
from jax.experimental import pallas as pl
from jax.experimental.pallas import tpu as pltpu
from jax.sharding import PartitionSpec as P


KVH = 2
HD = 128
LONGEST = 256


mom_decay = 0.9
step_size = 0.5


def rms_scale(values, gain):
    return values * lax.rsqrt(jnp.mean(values * values, axis=-1, keepdims=True) + 1e-06) * gain


def ring_order(count):
    return list(range(0, count, 2)) + list(range(count - 1 - count % 2, 0, -2))


def ring_gather(shard, axis, base, extra, beside):
    count = lax.axis_size(axis)
    order = ring_order(count)
    place = [0] * count
    for at, member in enumerate(order):
        place[member] = at
    ahead = [(order[i], order[(i + 1) % count]) for i in range(count)]
    back = [(b, a) for a, b in ahead]
    own = lax.axis_index(axis)
    here = jnp.asarray(place, jnp.int32)[own]
    ring = jnp.asarray(order, jnp.int32)
    rows, width = shard.shape
    half = rows // 2
    parts = [shard[:half], shard[half:]]
    full = lax.dynamic_update_slice(base, shard, (0, own * width))
    moving = {(way, part): parts[part] for way in (0, 1) for part in (0, 1)}
    there = ring[(here + jnp.arange(count)) % count]
    for step in range(1, count // 2 + 1):
        last = count // 2 - step
        fresh = []
        for part in (0, 1):
            for way in (0, 1):
                if step == count // 2 and way != part:
                    continue
                got = lax.ppermute(moving[way, part], axis, back if way else ahead)
                source = ring[(here + step if way else here - step) % count]
                fresh.append((way, part, got, source))
        if last in beside:
            extra = beside[last](extra, full, there)
            extra, *held = lax.optimization_barrier((extra, *[item[2] for item in fresh]))
            fresh = [(way, part, got, source) for (way, part, _, source), got in zip(fresh, held)]
        for way, part, got, source in fresh:
            moving[way, part] = got
            full = lax.dynamic_update_slice(full, got, (part * half, source * width))
    return full, extra, there


def listed_gather(shard, axis):
    order = ring_order(lax.axis_size(axis))
    return lax.all_gather(shard, axis, axis=1, tiled=True, axis_index_groups=[order])


def wide_pieces(shard, axis):
    count = lax.axis_size(axis)
    pieces = [shard]
    for k in range(1, count):
        bit = k & -k
        pieces.append(lax.ppermute(pieces[k & (k - 1)], axis, [(i, i ^ bit) for i in range(count)]))
    return pieces


def head_pieces(part, axis):
    count = lax.axis_size(axis)
    share = count // KVH
    split = share // 2
    own = lax.axis_index(axis)

    def source(head, q):
        return head * split + q if q < split else KVH * split + head * split + q - split

    got = []
    for turn in range(share):
        perm = [
            (source(head, (j + turn) % share), head * share + j)
            for head in range(KVH)
            for j in range(share)
        ]
        got.append(lax.ppermute(part, axis, perm))
    stacked = jnp.stack(got + got)
    ordered = lax.dynamic_slice_in_dim(stacked, (share - own % share) % share, share, 0)
    rows = part.shape[0]
    key = jnp.swapaxes(ordered[:split], 0, 1).reshape(rows, HD)
    value = jnp.swapaxes(ordered[split:], 0, 1).reshape(rows, HD)
    return key, value


def project(hidden, order, gain, query_weight, kv_weight, head_gains):
    tokens, features = hidden.shape
    cols = query_weight.shape[1]
    width = features // len(order)
    rows = math.gcd(tokens, 256)

    def body(hidden_ref, gain_ref, query_ref, kv_ref, head_ref, q_ref, k_ref, v_ref):
        total = jnp.zeros((rows, 1), jnp.float32)
        for at in range(len(order)):
            values = hidden_ref[:, at * width : (at + 1) * width].astype(jnp.float32)
            total = total + jnp.sum(values * values, axis=-1, keepdims=True)
        scale = lax.rsqrt(total / features + 1e-06)
        product = jnp.zeros((rows, cols), jnp.float32)
        keyval = jnp.zeros((rows, 2 * HD), jnp.float32)
        for at, member in enumerate(order):
            values = hidden_ref[:, at * width : (at + 1) * width].astype(jnp.float32)
            picked = slice(member * width, (member + 1) * width)
            normed = (values * scale * gain_ref[:, picked]).astype(jnp.bfloat16)
            product = product + jnp.dot(
                normed, query_ref[picked, :], preferred_element_type=jnp.float32
            )
            keyval = keyval + jnp.dot(
                normed, kv_ref[picked, :], preferred_element_type=jnp.float32
            )
        for head in range(cols // HD):
            lanes = slice(head * HD, (head + 1) * HD)
            q_ref[:, lanes] = rms_scale(product[:, lanes], head_ref[0:1, :]).astype(jnp.bfloat16)
        keyval = keyval.astype(jnp.bfloat16)
        v_ref[...] = keyval[:, HD:]
        key = keyval[:, :HD].astype(jnp.float32)
        k_ref[...] = rms_scale(key, head_ref[1:2, :]).astype(jnp.bfloat16)

    whole = lambda i: (0, 0)
    row = lambda i: (i, 0)
    return pl.pallas_call(
        body,
        grid=(tokens // rows,),
        in_specs=[
            pl.BlockSpec((rows, features), row),
            pl.BlockSpec((1, features), whole),
            pl.BlockSpec((features, cols), whole),
            pl.BlockSpec((features, 2 * HD), whole),
            pl.BlockSpec((2, HD), whole),
        ],
        out_specs=[
            pl.BlockSpec((rows, cols), row),
            pl.BlockSpec((rows, HD), row),
            pl.BlockSpec((rows, HD), row),
        ],
        out_shape=[
            jax.ShapeDtypeStruct((tokens, cols), jnp.bfloat16),
            jax.ShapeDtypeStruct((tokens, HD), jnp.bfloat16),
            jax.ShapeDtypeStruct((tokens, HD), jnp.bfloat16),
        ],
        cost_estimate=pl.CostEstimate(
            flops=2 * tokens * features * (cols + 2 * HD),
            transcendentals=0,
            bytes_accessed=2 * tokens * features,
        ),
        name="project",
    )(hidden, gain.reshape(1, features), query_weight, kv_weight, head_gains)


def attend(queries, key, value, segment):
    tokens, cols = queries.shape
    rows = math.gcd(tokens, LONGEST) if tokens % LONGEST else LONGEST
    assert rows == LONGEST

    def body(q_ref, k0_ref, k1_ref, v0_ref, v1_ref, col_ref, row0_ref, row1_ref, out_ref):
        at = pl.program_id(0)
        kept = []
        for back, (k_ref, row_ref) in ((1, (k0_ref, row0_ref)), (0, (k1_ref, row1_ref))):
            keys = k_ref[...]
            ours = lax.broadcasted_iota(jnp.int32, (rows, rows), 0)
            theirs = lax.broadcasted_iota(jnp.int32, (rows, rows), 1) - back * rows
            allowed = (ours >= theirs) & (theirs + at * rows >= 0) & (col_ref[...] == row_ref[...])
            kept.append((keys, allowed))
        for head in range(cols // HD):
            lanes = slice(head * HD, (head + 1) * HD)
            query = q_ref[:, lanes]
            scores = []
            for keys, allowed in kept:
                score = lax.dot_general(
                    query, keys, (((1,), (1,)), ((), ())), preferred_element_type=jnp.float32
                )
                scores.append(jnp.where(allowed, score * HD ** (-0.5), jnp.float32(-1e30)))
            highest = jnp.maximum(
                jnp.max(scores[0], axis=-1, keepdims=True),
                jnp.max(scores[1], axis=-1, keepdims=True),
            )
            expd = [jnp.exp(score - highest) for score in scores]
            norm = jnp.sum(expd[0], axis=-1, keepdims=True) + jnp.sum(
                expd[1], axis=-1, keepdims=True
            )
            probs = [(e / norm).astype(jnp.bfloat16) for e in expd]
            context = jnp.dot(
                probs[0], v0_ref[...], preferred_element_type=jnp.float32
            ) + jnp.dot(probs[1], v1_ref[...], preferred_element_type=jnp.float32)
            out_ref[:, lanes] = context.astype(jnp.bfloat16)

    before = lambda i: (jnp.maximum(i - 1, 0), 0)
    current = lambda i: (i, 0)
    before_row = lambda i: (0, jnp.maximum(i - 1, 0))
    current_row = lambda i: (0, i)
    return pl.pallas_call(
        body,
        grid=(tokens // rows,),
        in_specs=[
            pl.BlockSpec((rows, cols), current),
            pl.BlockSpec((rows, HD), before),
            pl.BlockSpec((rows, HD), current),
            pl.BlockSpec((rows, HD), before),
            pl.BlockSpec((rows, HD), current),
            pl.BlockSpec((rows, 1), current),
            pl.BlockSpec((1, rows), before_row),
            pl.BlockSpec((1, rows), current_row),
        ],
        out_specs=pl.BlockSpec((rows, cols), current),
        out_shape=jax.ShapeDtypeStruct((tokens, cols), jnp.bfloat16),
        cost_estimate=pl.CostEstimate(
            flops=32 * tokens * rows * cols, transcendentals=0, bytes_accessed=4 * tokens * cols
        ),
        name="attend",
    )(
        queries,
        key,
        key,
        value,
        value,
        segment.reshape(tokens, 1),
        segment.reshape(1, tokens),
        segment.reshape(1, tokens),
    )


def predict(feat, places, table, joined, first, base, target=None, valid=None):
    tokens = feat.shape[0]
    steps = table.shape[0]
    inner = feat.shape[1] // lax.axis_size("narrow")
    cols = joined.shape[1]
    ends = target is not None

    def body(places_ref, table_ref, *refs):
        at = pl.program_id(0)
        feat_ref, joined_ref = refs[:2]
        out_ref = refs[-2] if ends else refs[-1]
        product = jnp.dot(feat_ref[...], joined_ref[...], preferred_element_type=jnp.float32)

        @pl.when(at == 0)
        def _():
            out_ref[...] = product if base is None else refs[2][...] + product

        @pl.when(at > 0)
        def _():
            out_ref[...] += product

        if ends:

            @pl.when(at == steps - 1)
            def _():
                error = (out_ref[...] - refs[3][...].astype(jnp.float32)) * refs[4][...]
                out_ref[...] = error
                refs[-1][...] = error.astype(jnp.bfloat16)

    whole = lambda i, places_ref, table_ref: (0, 0)
    in_specs = [
        pl.BlockSpec((tokens, inner), lambda i, places_ref, table_ref: (0, places_ref[i])),
        pl.BlockSpec(
            (inner, cols), lambda i, places_ref, table_ref: (first // inner + table_ref[i], 0)
        ),
    ]
    operands = [feat, joined]
    if base is not None:
        in_specs.append(pl.BlockSpec((tokens, cols), whole))
        operands.append(base)
    out_specs = pl.BlockSpec((tokens, cols), whole)
    out_shape = jax.ShapeDtypeStruct((tokens, cols), jnp.float32)
    if ends:
        in_specs += [pl.BlockSpec((tokens, cols), whole), pl.BlockSpec((tokens, 1), whole)]
        operands += [target, valid.reshape(tokens, 1)]
        out_specs = [out_specs, pl.BlockSpec((tokens, cols), whole)]
        out_shape = [out_shape, jax.ShapeDtypeStruct((tokens, cols), jnp.bfloat16)]
    return pl.pallas_call(
        body,
        grid_spec=pltpu.PrefetchScalarGridSpec(
            num_scalar_prefetch=2, grid=(steps,), in_specs=in_specs, out_specs=out_specs
        ),
        out_shape=out_shape,
        cost_estimate=pl.CostEstimate(
            flops=2 * tokens * steps * inner * cols,
            transcendentals=0,
            bytes_accessed=2 * tokens * steps * inner,
        ),
        name="predict",
    )(places, table, *operands)


def grad_rows(first, pieces, parts, width, tables, feats, errors, out_dtype):
    per = tables[0].shape[0]
    kinds = len(tables)
    tokens, cols = errors[0].shape
    each = pieces // parts

    def body(first_ref, table_ref, *refs):
        out_refs = refs[-parts:]
        error_refs = refs[-parts - len(errors) : -parts]
        piece = first_ref[0] + pl.program_id(0)
        for at in range(kinds):

            @pl.when(piece // per == at)
            def _(at=at):
                total = None
                for group, error_ref in enumerate(error_refs):
                    term = lax.dot_general(
                        refs[group * kinds + at][...],
                        error_ref[...],
                        (((0,), (0,)), ((), ())),
                        preferred_element_type=jnp.float32,
                    )
                    total = term if total is None else total + term
                for part, out_ref in enumerate(out_refs):

                    @pl.when(pl.program_id(0) // each == part)
                    def _(out_ref=out_ref):
                        out_ref[...] = total.astype(out_dtype)

    def out_map(part):
        return lambda i, first_ref, table_ref: (jnp.clip(i - part * each, 0, each - 1), 0)

    def feat_map(at):
        def of(i, first_ref, table_ref):
            piece = jnp.clip(first_ref[0] + i - at * per, 0, per - 1)
            return (0, table_ref[at * per + piece])

        return of

    whole = lambda i, first_ref, table_ref: (0, 0)
    in_specs = [
        pl.BlockSpec((tokens, width), feat_map(at)) for _ in errors for at in range(kinds)
    ]
    in_specs += [pl.BlockSpec((tokens, cols), whole) for _ in errors]
    return pl.pallas_call(
        body,
        grid_spec=pltpu.PrefetchScalarGridSpec(
            num_scalar_prefetch=2,
            grid=(pieces,),
            in_specs=in_specs,
            out_specs=[pl.BlockSpec((width, cols), out_map(part)) for part in range(parts)],
        ),
        out_shape=[jax.ShapeDtypeStruct((each * width, cols), out_dtype)] * parts,
        cost_estimate=pl.CostEstimate(
            flops=4 * tokens * pieces * width * cols,
            transcendentals=0,
            bytes_accessed=4 * tokens * pieces * width,
        ),
        name="grad_rows",
    )(first.reshape(1), jnp.concatenate(tables), *[f for group in feats for f in group], *errors)


def update(grads, far, joining, momentum, part, outs, tokens):
    rows, cols = far[0].shape
    step = math.gcd(rows, 256)
    skip = part * (rows // step)

    def body(grads_ref, joining_ref, momentum_ref, *refs):
        total = grads_ref[...]
        for far_ref in refs[: len(far)]:
            total = total + far_ref[...].astype(jnp.float32)
        fresh = mom_decay * momentum_ref[...] + total / tokens
        refs[-2][...] = joining_ref[...] - step_size * fresh
        refs[-1][...] = fresh

    here = pl.BlockSpec((step, cols), lambda i: (skip + i, 0))
    own = pl.BlockSpec((step, cols), lambda i: (i, 0))
    shape = jax.ShapeDtypeStruct(joining.shape, jnp.float32)
    return pl.pallas_call(
        body,
        grid=(rows // step,),
        in_specs=[here] * 3
        + [own] * len(far)
        + [pl.BlockSpec(memory_space=pl.ANY)] * len(outs),
        out_specs=[here, here],
        out_shape=[shape, shape],
        input_output_aliases={3 + len(far) + at: at for at in range(len(outs))},
        cost_estimate=pl.CostEstimate(
            flops=6 * rows * cols, transcendentals=0, bytes_accessed=22 * rows * cols
        ),
        name="update",
    )(grads, joining, momentum, *far, *outs)


def step_on_device(
    resid_in,
    low_feat,
    mid_feat,
    segment,
    assign,
    attn_gain,
    qk_gain,
    query_weight,
    kv_weight,
    out_weight,
    joining_weight,
    momentum,
):
    groups = lax.axis_size("wide")
    narrow = lax.axis_size("narrow")
    mine = lax.axis_index("wide").astype(jnp.int32)
    tokens_local = resid_in.shape[0]
    block = tokens_local // groups
    features = query_weight.shape[0]
    width = features // narrow
    order = ring_order(narrow)
    partner = [(i, i ^ 1) for i in range(groups)]

    hidden_full = listed_gather(resid_in, "narrow")
    low_full = listed_gather(low_feat, "narrow")
    mid_full = listed_gather(mid_feat, "narrow")

    share = out_weight.shape[0] // groups
    rows_mine = lax.dynamic_slice_in_dim(out_weight, mine * share, share, 0)
    got = lax.all_to_all(rows_mine, "narrow", split_axis=1, concat_axis=0, tiled=True)
    out_pieces = wide_pieces(got, "wide")
    rows_here = joining_weight.shape[0]
    joined_pieces = wide_pieces(joining_weight.astype(jnp.bfloat16), "wide")

    kv_share = features // groups
    kv_rows = lax.dynamic_slice_in_dim(kv_weight, mine * kv_share, kv_share, 0)
    kv_rows = jnp.concatenate(head_pieces(kv_rows, "narrow"), axis=1)
    kv_own = jnp.zeros((features, 2 * HD), kv_weight.dtype)
    for k, piece in enumerate(wide_pieces(kv_rows, "wide")):
        kv_own = lax.dynamic_update_slice(kv_own, piece, ((mine ^ k) * kv_share, 0))

    hidden_full, kv_own, joined_pieces, out_pieces = lax.optimization_barrier(
        (hidden_full, kv_own, joined_pieces, out_pieces)
    )
    out_cols = jnp.zeros((narrow, groups, share, width), out_weight.dtype)
    for k, piece in enumerate(out_pieces):
        out_cols = lax.dynamic_update_slice(
            out_cols, piece.reshape(narrow, 1, share, width), (0, mine ^ k, 0, 0)
        )
    out_cols = out_cols.reshape(narrow * groups * share, width)
    joined = jnp.zeros((rows_here * groups, joining_weight.shape[1]), jnp.bfloat16)
    for k, piece in enumerate(joined_pieces):
        joined = lax.dynamic_update_slice(joined, piece, ((mine ^ k) * rows_here, 0))

    queries, key, value = project(
        hidden_full, order, attn_gain, query_weight, kv_own, qk_gain
    )
    context = attend(queries, key, value, segment)

    listed = jnp.asarray(order, jnp.int32)
    natural = jnp.arange(narrow, dtype=jnp.int32)
    low_other = lax.ppermute(low_full, "wide", partner)
    mid_other = lax.ppermute(mid_full, "wide", partner)

    def of_low(pred, full, there):
        return predict(low_full, natural, listed, joined, 0, None)

    def of_mid(pred, full, there):
        return predict(mid_full, natural, listed, joined, features, pred)

    def of_high(pred, full, there):
        near = jnp.concatenate([there[: narrow // 2], there[narrow // 2 + 1 :]])
        return predict(full, near, near, joined, 2 * features, pred)

    context_full, pred, _ = ring_gather(context, "narrow", hidden_full, None, {1: of_low})
    attn_cols = jnp.dot(context_full, out_cols, preferred_element_type=jnp.float32)
    high = resid_in.astype(jnp.float32) + attn_cols
    valid = jnp.concatenate(
        [(segment[1:] == segment[:-1]).astype(jnp.float32), jnp.zeros((1,), jnp.float32)]
    )
    target = (
        jnp.concatenate([high[1:], jnp.zeros((1, high.shape[1]), jnp.float32)], axis=0)
        * valid[:, None]
    ).astype(jnp.bfloat16)
    high_full, pred, there = ring_gather(
        high.astype(jnp.bfloat16), "narrow", context_full, pred, {1: of_mid, 0: of_high}
    )
    last = there[narrow // 2 : narrow // 2 + 1]
    high_other = lax.ppermute(high_full, "wide", partner)

    error, error_bf = predict(
        high_full, last, last, joined, 2 * features, pred, target, valid
    )
    error_other = lax.ppermute(error_bf, "wide", partner)

    own_row = assign[mine]
    slots = jnp.arange(groups, dtype=jnp.int32)
    inverse = jnp.sum(jnp.where(own_row[None, :] == slots[:, None], slots[None, :], 0), axis=1)
    sent = []
    for k in sorted(range(groups), key=lambda k: -k):
        piece = lax.dynamic_slice_in_dim(error, inverse[mine ^ k] * block, block, 0)
        if k > 1:
            piece = piece.astype(jnp.bfloat16)
        if k:
            piece = lax.ppermute(piece, "wide", [(i, i ^ k) for i in range(groups)])
        sent.append((k, piece))

    place = jnp.asarray([order.index(member) for member in range(narrow)], jnp.int32)
    tables = (place, place, natural)
    feats = ((low_full, mid_full, high_full), (low_other, mid_other, high_other))
    per_chunk = rows_here // width

    def rows_of(member, start, pieces, dtype):
        (rows,) = grad_rows(
            member * per_chunk + start,
            pieces,
            1,
            width,
            tables,
            feats,
            (error_bf, error_other),
            dtype,
        )
        return rows

    parts = 2
    each = per_chunk // parts
    far = []
    for bit in range(2, groups, 2):
        moved = []
        for part in range(parts):
            away = rows_of(mine ^ bit, part * each, each, jnp.bfloat16)
            moved.append(lax.ppermute(away, "wide", [(i, i ^ bit) for i in range(groups)]))
        far.append(moved)
    grads = rows_of(mine, 0, per_chunk, jnp.float32)
    error_out = jnp.zeros_like(error)
    for k, piece in sent:
        error_out = lax.dynamic_update_slice(
            error_out, piece.astype(jnp.float32), ((mine ^ k) * block, 0)
        )
    outs = ()
    for part in range(parts):
        pieces = [moved[part] for moved in far]
        outs = update(
            grads, pieces, joining_weight, momentum, part, outs, tokens_local * groups
        )
    new_joining, new_momentum = outs
    return (error_out, new_joining, new_momentum)


def solution(mesh):
    placed = (
        P("wide", "narrow"),
        P("wide", "narrow"),
        P("wide", "narrow"),
        P("wide"),
        P(),
        P(),
        P(),
        P(None, "narrow"),
        P(None, "narrow"),
        P("narrow", None),
        P("wide", "narrow"),
        P("wide", "narrow"),
    )
    return jax.shard_map(
        step_on_device,
        mesh=mesh,
        in_specs=placed,
        out_specs=(P("wide", "narrow"), P("wide", "narrow"), P("wide", "narrow")),
        check_vma=False,
    )
```
